32 devices in a mesh: sector: 4 (over y, x), term: 8 (over z, core).
Axes of the slice: x: 2, y: 2, z: 4, core: 2. Of those that a mesh axis runs over, the one named last changes fastest.
Arguments:
- wavefunction: bfloat16 [256, 4, 2, 256], P('term', 'sector'), may hold values from -6 to 6
- left_ops: bfloat16 [128, 4, 256, 256], P('term', 'sector'), may hold values from -0.5 to 0.5
- right_ops: bfloat16 [128, 4, 256, 256], P('term', 'sector'), may hold values from -0.03125 to 0.03125
- op_scales: float32 [128, 4], P('term', 'sector'), may hold values from 0.5 to 2
- sources: int32 [128, 4], P('term', 'sector'), may hold values from 0 to 1
- coupled_sectors: int32 [4, 2], P('sector'), may hold values from 0 to 3, as said below
- left_dims: int32 [4], replicated, may hold values from 1 to 256, 768 in all
- right_dims: int32 [4], replicated, may hold values from 1 to 256, 768 in all
Outputs:
- sigma: bfloat16 [256, 4, 2, 256], P('term', 'sector')
The draws below stay inside these ranges and needn't reach their ends.
Inputs may be any that keep to these rules, and one draw needn't show every extreme that they name: `coupled_sectors`: the 2 sectors of each row are distinct. `left_dims`: the sizes of all sectors add up to 768. `right_dims`: the sizes of all sectors add up to 768.
All inputs are finite; a program needn't handle non-finite values.
Results may differ from the reference program's by a relative error of at most 0.025.
Values may be sent and summed in bfloat16 or wider, within the bound.
No kernel may reach another device: no remote copies, remote signals or barrier semaphores. Data moves between devices by JAX's collectives and lax.ppermute only.
A program may use at most 64 MiB of HBM per device.

```python
import math
import jax
import jax.numpy as jnp
import numpy as np
from jax import lax

M = 256
NVEC = 2
SEC = 4
COUPLED = 2
TERMS = 128


def draw_coupled_sectors(key, part):

    def one_row(row):
        return jax.random.permutation(jax.random.fold_in(key, row + 7), SEC)[:COUPLED]
    return jax.vmap(one_row)(jnp.arange(SEC)).astype(jnp.int32)


def place_ends(array, own_key, least, top_value):
    index_at = [jax.random.randint(jax.random.fold_in(own_key, axis), (), 0, length) for axis, length in enumerate(array.shape)]
    longest = array.shape.index(max(array.shape))
    next_to = index_at[:longest] + [(index_at[longest] + 1) % array.shape[longest]] + index_at[longest + 1:]
    return array.at[tuple(index_at)].set(least).at[tuple(next_to)].set(top_value)


def with_spikes(entries, own_key, source, target, parts, factor):
    def block_of(dim):
        return (jnp.arange(entries.shape[dim]) // (entries.shape[dim] // parts)).reshape((-1,) + (1,) * (entries.ndim - 1 - dim))

    first = jax.random.permutation(own_key, parts)[block_of(target)]
    second = (block_of(target) + parts // 2) % parts
    return jnp.where((block_of(source) == first) | (block_of(source) == second), factor * entries, entries)


def levels(key, extent, split, least, high):
    def one(dim, blocks):
        draws = jax.random.uniform(jax.random.fold_in(jax.random.fold_in(key, 6), dim), (blocks,), jnp.float32, least / len(split), high / len(split))
        return jnp.repeat(jnp.exp(draws), extent[dim] // blocks).reshape((-1,) + (1,) * (len(extent) - dim - 1))

    factor_of = one(*split[0])
    for cut in split[1:]:
        factor_of = factor_of * one(*cut)
    return factor_of


def profile(number_of, total, reach, lean):
    weights = [(1 << 20) // math.isqrt(grade ** lean) + 1 for grade in range(2, number_of + 1)]
    surplus, given = total - reach - (number_of - 1), [1] * (number_of - 1)
    while surplus > 0:
        free = [i for i in range(number_of - 1) if given[i] < reach]
        pool, remaining = sum([weights[i] for i in free]), surplus
        for i in free:
            addition = min(reach - given[i], max(1, remaining * weights[i] // pool), surplus)
            given[i] = given[i] + addition
            surplus = surplus - addition
    return np.array([reach] + given)


def ragged(own_key, count, total, bound, slope):
    if count == 2:
        one = jax.random.randint(own_key, (), max(1, total - bound), min(bound, total - 1) + 1)
        return jnp.stack([one, total - one])
    lengths = jnp.asarray(profile(count, total, bound, slope), jnp.int32)
    couples = (count - 1) // 2
    donor, taker = lengths[1:1 + 2 * couples:2], lengths[2:2 + 2 * couples:2]
    margin = jnp.minimum(donor - 1, bound - taker)
    passed = jax.random.randint(jax.random.fold_in(own_key, 1), (couples,), 0, 1 << 20) % (margin + 1)
    lengths = lengths.at[1:1 + 2 * couples:2].set(donor - passed).at[2:2 + 2 * couples:2].set(taker + passed)
    return lengths[jax.random.permutation(jax.random.fold_in(own_key, 2), count)]


def bell_draw(key, shape, scale, bound, cuts=(), kind=jnp.bfloat16):
    array = jax.random.normal(key, shape, jnp.float32) * scale
    if len(cuts) > 0:
        array = levels(key, shape, cuts, -0.22, 0.18) * array
    return jnp.clip(array, min=-bound, max=bound).astype(kind)


def bell_draw_with(stream_key, shape, deviation, bound, split, heavy, kind=jnp.bfloat16):
    array = deviation * jax.random.normal(stream_key, shape, jnp.float32)
    if split:
        array = array * levels(stream_key, shape, split, -0.22, 0.18)
    return jnp.clip(with_spikes(array, jax.random.fold_in(stream_key, 3), *heavy), -bound, bound).astype(kind)


def setup_inputs(seed: int = 0) -> dict:
    streams_of = jax.random.split(jax.random.key(seed), 9)
    wavefunction = bell_draw(streams_of[0], (M, SEC, NVEC, M), 1.0, 6.0, ((0, 8), (1, 4)))
    left_ops = bell_draw_with(streams_of[1], (TERMS, SEC, M, M), M ** -0.5, 0.5, ((0, 8), (1, 4)), (0, 2, 8, 2.0))
    right_ops = bell_draw(streams_of[2], (TERMS, SEC, M, M), (M * TERMS) ** -0.5, 0.03125, ((0, 8), (1, 4)))
    op_scales = jnp.clip(jnp.exp(math.log(2.0) - 1.3862944 * jax.random.uniform(streams_of[3], (TERMS, SEC), jnp.float32) ** levels(streams_of[3], (TERMS, SEC), ((0, 8), (1, 4)), -0.2, 0.2)), 0.5, 2.0)
    sources = place_ends(jax.random.randint(streams_of[4], (TERMS, SEC), 0, COUPLED), jax.random.fold_in(streams_of[4], 1), 0, COUPLED - 1).astype(jnp.int32)
    coupled_sectors = draw_coupled_sectors(jax.random.fold_in(streams_of[8], 71), 0)
    left_dims = ragged(streams_of[6], SEC, SEC * M * 3 // 4, M, 1).astype(jnp.int32)
    right_dims = ragged(streams_of[7], SEC, SEC * M * 3 // 4, M, 1).astype(jnp.int32)
    return dict(wavefunction=wavefunction, left_ops=left_ops, right_ops=right_ops, op_scales=op_scales, sources=sources, coupled_sectors=coupled_sectors, left_dims=left_dims, right_dims=right_dims)


def live_mask(states, sectors, left_dims, right_dims):
    row_index = lax.broadcasted_iota(jnp.int32, (states, sectors), 0)
    col_index = lax.broadcasted_iota(jnp.int32, (sectors, states), 1)
    row_ok = row_index < left_dims[None, :]
    col_ok = col_index < right_dims[:, None]
    return row_ok[:, :, None, None] & col_ok[None, :, None, :]


def reference(wavefunction, left_ops, right_ops, op_scales, sources, coupled_sectors, left_dims, right_dims):
    states = wavefunction.shape[0]
    sectors = wavefunction.shape[1]
    present = live_mask(states, sectors, left_dims, right_dims)
    masked = jnp.where(present, wavefunction, jnp.zeros((), wavefunction.dtype))
    table = jnp.broadcast_to(coupled_sectors[None, :, :], (sources.shape[0], sectors, coupled_sectors.shape[1]))
    chosen = jnp.take_along_axis(table, sources[:, :, None].astype(jnp.int32), axis=2)[:, :, 0].astype(jnp.int32)

    def one_term(accum, pieces):
        left_block, right_block, scales, picks = pieces
        picked = jnp.take(masked, picks, axis=1)
        product = jnp.einsum("sij,jsvk->isvk", left_block.astype(jnp.float32), picked.astype(jnp.float32))
        product = product.astype(jnp.bfloat16)
        contrib = jnp.einsum("isvk,skl->isvl", product.astype(jnp.float32), right_block.astype(jnp.float32))
        return accum + contrib * scales[None, :, None, None], None

    starting = jnp.zeros((states, sectors, NVEC, states), jnp.float32)
    summed, unused = lax.scan(one_term, starting, (left_ops, right_ops, op_scales, chosen))
    return jnp.where(present, summed, jnp.zeros((), jnp.float32)).astype(jnp.bfloat16)
```

```python
import functools

import jax
import jax.numpy as jnp
from jax import lax
from jax.experimental import pallas as pl
from jax.experimental.pallas import tpu as pltpu
from jax.sharding import PartitionSpec as P

VMEM = pltpu.VMEM
SMEM = pltpu.SMEM


def swap(x, axis, size, mask):
    return lax.ppermute(x, axis, [(i, i ^ mask) for i in range(size)])


def pick_kernel(count, place_ref, coupled_ref, left_ref, right_ref, *refs):
    blocks, out_ref = refs[:count], refs[count]
    me, first_row = place_ref[0], place_ref[1]
    vectors, rows, states = out_ref.shape[1:]
    row = lax.broadcasted_iota(jnp.int32, (rows, states), 0) + first_row
    col = lax.broadcasted_iota(jnp.int32, (rows, states), 1)
    for c in range(out_ref.shape[0]):
        sector = coupled_ref[0, c]
        which = sector ^ me
        live = (row < left_ref[sector]) & (col < right_ref[sector])
        for v in range(vectors):
            value = blocks[0][:, 0, v, :].astype(jnp.float32)
            for m in range(1, count):
                value = jnp.where(which == m, blocks[m][:, 0, v, :].astype(jnp.float32), value)
            out_ref[c, v] = jnp.where(live, value, 0.0).astype(out_ref.dtype)


def contract(scale_ref, source_ref, left_ref, right_ref, psi_ref, prod_ref):
    terms, _, states, _ = left_ref.shape
    vectors = psi_ref.shape[2] // states
    for t in range(terms):
        prod = jnp.dot(left_ref[t, 0], psi_ref[source_ref[t, 0]], preferred_element_type=jnp.float32)
        prod = (prod * scale_ref[t, 0]).astype(jnp.bfloat16)
        for v in range(vectors):
            prod_ref[v * states:(v + 1) * states, t * states:(t + 1) * states] = (
                prod[:, v * states:(v + 1) * states])
    return jnp.dot(prod_ref[...], right_ref[...].reshape(terms * states, states),
                   preferred_element_type=jnp.float32)


def sigma_kernel(chips, place_ref, scale_ref, source_ref, left_ref, right_ref, *refs):
    blocks = refs[:2 * chips]
    send_ref, keep_ref, psi_ref, prod_ref = refs[2 * chips:]
    chip, core = place_ref[0], place_ref[1]
    coupled, vectors, rows, states = blocks[0].shape
    for n, block in enumerate(blocks):
        owner = ((chip ^ (n % chips)) * 2) + (core ^ (n // chips))
        start = pl.multiple_of(owner * rows, rows)
        for c in range(coupled):
            for v in range(vectors):
                psi_ref[c, pl.ds(start, rows), v * states:(v + 1) * states] = block[c, v]
    total = contract(scale_ref, source_ref, left_ref, right_ref, psi_ref, prod_ref)
    for z in range(chips):
        for v in range(vectors):
            base = v * states + 2 * z * rows
            even, odd = total[base:base + rows], total[base + rows:base + 2 * rows]
            mine = jnp.where(core == 0, even, odd)
            other = jnp.where(core == 0, odd, even)
            keep_ref[z, v] = mine
            send_ref[z, v] = other.astype(send_ref.dtype)


def split_kernel(chips, place_ref, keep_ref, recv_ref, *outs):
    chip = place_ref[0]
    for n in range(chips):
        at = chip ^ n
        outs[n][...] = (keep_ref[at] + recv_ref[at].astype(jnp.float32)).astype(outs[n].dtype)


def call(kernel, outs, smem, vmem, args, scratch=(), **params):
    return pl.pallas_call(
        kernel,
        out_shape=outs,
        in_specs=[pl.BlockSpec(memory_space=SMEM)] * smem + [pl.BlockSpec(memory_space=VMEM)] * vmem,
        out_specs=jax.tree.map(lambda _: pl.BlockSpec(memory_space=VMEM), outs),
        scratch_shapes=list(scratch),
        compiler_params=pltpu.CompilerParams(**params),
    )(*args)


def direct(wave, left_ops, right_ops, op_scales, sources, coupled, left_dims, right_dims):
    sectors, term_devices = lax.axis_size("sector"), lax.axis_size("term")
    chips = term_devices // 2
    rows, _, vectors, states = wave.shape
    terms, chosen = left_ops.shape[0], coupled.shape[1]
    me, place = lax.axis_index("sector"), lax.axis_index("term")
    chip, core = place // 2, place % 2
    bf16, f32 = jnp.bfloat16, jnp.float32

    shares = [wave] + [swap(wave, "sector", sectors, m) for m in range(1, sectors)]
    spot = jnp.stack([me, place * rows]).astype(jnp.int32)
    own = call(functools.partial(pick_kernel, sectors),
               jax.ShapeDtypeStruct((chosen, vectors, rows, states), bf16),
               4, sectors, (spot, coupled, left_dims, right_dims, *shares))
    line = [own] + [swap(own, "term", term_devices, 2 * m) for m in range(1, chips)]
    line = line + [swap(b, "term", term_devices, 1) for b in line]
    seat = jnp.stack([chip, core]).astype(jnp.int32)
    send, keep = call(functools.partial(sigma_kernel, chips),
                      (jax.ShapeDtypeStruct((chips, vectors, rows, states), bf16),
                       jax.ShapeDtypeStruct((chips, vectors, rows, states), f32)),
                      3, 2 + len(line), (seat, op_scales, sources, left_ops, right_ops, *line),
                      (VMEM((chosen, states, vectors * states), bf16),
                       VMEM((vectors * states, terms * states), bf16)))
    parts = call(functools.partial(split_kernel, chips),
                 (jax.ShapeDtypeStruct((vectors, rows, states), f32),)
                 + (jax.ShapeDtypeStruct((vectors, rows, states), bf16),) * (chips - 1),
                 1, 2, (seat, keep, swap(send, "term", term_devices, 1)))
    total = parts[0]
    for m in range(1, chips):
        total = total + swap(parts[m], "term", term_devices, 2 * m).astype(f32)
    row = lax.broadcasted_iota(jnp.int32, (1, rows, states), 1) + place * rows
    col = lax.broadcasted_iota(jnp.int32, (1, rows, states), 2)
    live = (row < left_dims[me]) & (col < right_dims[me])
    total = jnp.where(live, total, 0.0).astype(bf16)
    return jnp.transpose(total, (1, 0, 2))[:, None]


def whole_kernel(scale_ref, source_ref, left_ref, right_ref, blocks_ref, out_ref, prod_ref):
    out_ref[...] = contract(scale_ref, source_ref, left_ref, right_ref, blocks_ref, prod_ref)


def gathered(wave, left_ops, right_ops, op_scales, sources, coupled, left_dims, right_dims):
    rows, _, vectors, states = wave.shape
    terms, chosen = left_ops.shape[0], coupled.shape[1]
    me, place = lax.axis_index("sector"), lax.axis_index("term")
    shares = lax.all_gather(wave[:, 0], "sector", axis=0)
    picks = coupled[0]
    row = lax.broadcasted_iota(jnp.int32, (1, rows, 1, states), 1) + place * rows
    col = lax.broadcasted_iota(jnp.int32, (1, rows, 1, states), 3)
    live = ((row < jnp.take(left_dims, picks)[:, None, None, None])
            & (col < jnp.take(right_dims, picks)[:, None, None, None]))
    own = jnp.where(live, jnp.take(shares, picks, axis=0), jnp.zeros((), wave.dtype))
    blocks = lax.all_gather(own, "term", axis=1, tiled=True).reshape(chosen, -1, vectors * states)
    total = call(whole_kernel, jax.ShapeDtypeStruct((vectors * states, states), jnp.float32),
                 2, 3, (op_scales, sources, left_ops, right_ops, blocks),
                 (VMEM((vectors * states, terms * states), jnp.bfloat16),))
    total = jnp.transpose(total.reshape(vectors, states, states), (1, 0, 2))
    row = lax.broadcasted_iota(jnp.int32, total.shape, 0)
    col = lax.broadcasted_iota(jnp.int32, total.shape, 2)
    total = jnp.where((row < left_dims[me]) & (col < right_dims[me]), total, 0.0)
    return lax.psum_scatter(total.astype(jnp.bfloat16), "term", scatter_dimension=0, tiled=True)[:, None]


def solution(mesh):
    in_specs = (
        P("term", "sector", None, None),
        P("term", "sector", None, None),
        P("term", "sector", None, None),
        P("term", "sector"),
        P("term", "sector"),
        P("sector", None),
        P(),
        P(),
    )
    out_specs = P("term", "sector", None, None)
    small = mesh.shape["sector"] == 4 and mesh.shape["term"] == 8
    return jax.shard_map(direct if small else gathered, mesh=mesh, in_specs=in_specs,
                         out_specs=out_specs, check_vma=False)
```

```python
import functools

import jax
import jax.numpy as jnp
from jax import lax
from jax.experimental import pallas as pl
from jax.experimental.pallas import tpu as pltpu
from jax.sharding import PartitionSpec as P

VMEM = pltpu.VMEM
SMEM = pltpu.SMEM


def swap(x, axis, size, mask):
    return lax.ppermute(x, axis, [(i, i ^ mask) for i in range(size)])


def load_kernel(sectors, coupled_ref, left_ref, right_ref, wave_ref, ops_ref, coops_ref, scale_ref, source_ref,
                ops_out, coops_out, scale_out, source_out, own_out, masks_out, live_out, wave_vmem, sems):
    copies = [pltpu.make_async_copy(src, dst, sems.at[n]) for n, (src, dst) in enumerate((
        (wave_ref, wave_vmem), (ops_ref, ops_out), (coops_ref, coops_out),
        (scale_ref, scale_out), (source_ref, source_out)))]
    for copy in copies:
        copy.start()
    chosen, vectors, rows, states = own_out.shape
    me, first_row = lax.axis_index("sector"), lax.axis_index("term") * rows
    row = lax.broadcasted_iota(jnp.int32, (rows, states), 0) + first_row
    col = lax.broadcasted_iota(jnp.int32, (rows, states), 1)
    live_out[...] = ((row < left_ref[me]) & (col < right_ref[me])).astype(jnp.float32)
    for c in range(chosen):
        sector = coupled_ref[0, c]
        live = ((row < left_ref[sector]) & (col < right_ref[sector])).astype(jnp.float32)
        for m in range(sectors):
            masks_out[c, m] = jnp.where((sector ^ me) == m, live, 0.0)
    copies[0].wait()
    for v in range(vectors):
        value = wave_vmem[:, 0, v, :].astype(jnp.float32)
        for c in range(chosen):
            own_out[c, v] = masks_out[c, 0] * value
    for copy in copies[1:]:
        copy.wait()


def pick_kernel(masks_ref, own_ref, *refs):
    blocks, out_ref = refs[:-1], refs[-1]
    chosen, vectors = out_ref.shape[:2]
    for v in range(vectors):
        values = [block[:, 0, v, :].astype(jnp.float32) for block in blocks]
        for c in range(chosen):
            total = own_ref[c, v]
            for m, value in enumerate(values):
                total = total + masks_ref[c, m + 1] * value
            out_ref[c, v] = total.astype(out_ref.dtype)


def contract(scale_ref, source_ref, left_ref, right_ref, psi_ref, prod_ref):
    terms, _, states, _ = left_ref.shape
    vectors = psi_ref.shape[2] // states
    for t in range(terms):
        prod = jnp.dot(left_ref[t, 0], psi_ref[source_ref[t]], preferred_element_type=jnp.float32)
        prod = (prod * scale_ref[t]).astype(jnp.bfloat16)
        for v in range(vectors):
            prod_ref[v * states:(v + 1) * states, t * states:(t + 1) * states] = (
                prod[:, v * states:(v + 1) * states])
    return jnp.dot(prod_ref[...], right_ref[...].reshape(terms * states, states),
                   preferred_element_type=jnp.float32)


def sigma_kernel(chips, scale_ref, source_ref, left_ref, right_ref, *refs):
    blocks = refs[:2 * chips]
    send_ref, keep_ref, psi_ref, prod_ref = refs[2 * chips:]
    place = lax.axis_index("term")
    chip, core = place >> 1, place & 1
    coupled, vectors, rows, states = blocks[0].shape
    for n, block in enumerate(blocks):
        owner = ((chip ^ (n % chips)) * 2) + (core ^ (n // chips))
        start = pl.multiple_of(owner * rows, rows)
        for c in range(coupled):
            for v in range(vectors):
                psi_ref[c, pl.ds(start, rows), v * states:(v + 1) * states] = block[c, v]
    total = contract(scale_ref, source_ref, left_ref, right_ref, psi_ref, prod_ref)
    for z in range(chips):
        for v in range(vectors):
            base = v * states + 2 * z * rows
            even, odd = total[base:base + rows], total[base + rows:base + 2 * rows]
            mine = jnp.where(core == 0, even, odd)
            other = jnp.where(core == 0, odd, even)
            keep_ref[z, v] = mine
            send_ref[z, v] = other.astype(send_ref.dtype)


def split_kernel(chips, keep_ref, recv_ref, *outs):
    chip = lax.axis_index("term") >> 1
    for n in range(chips):
        at = chip ^ n
        outs[n][...] = (keep_ref[at] + recv_ref[at].astype(jnp.float32)).astype(outs[n].dtype)


def call(kernel, outs, smem, vmem, args, scratch=()):
    args = args[:smem] + tuple(pltpu.with_memory_space_constraint(x, VMEM) for x in args[smem:])
    return pl.pallas_call(
        kernel,
        out_shape=outs,
        in_specs=[pl.BlockSpec(memory_space=SMEM)] * smem + [pl.BlockSpec(memory_space=VMEM)] * vmem,
        out_specs=jax.tree.map(lambda _: pl.BlockSpec(memory_space=VMEM), outs),
        scratch_shapes=list(scratch),
        compiler_params=pltpu.CompilerParams(vmem_limit_bytes=24 << 20),
    )(*args)


def final_kernel(live_ref, total_ref, *refs):
    parts, out_ref = refs[:-1], refs[-1]
    for v in range(total_ref.shape[0]):
        total = total_ref[v]
        for part in parts:
            total = total + part[v].astype(jnp.float32)
        out_ref[:, 0, v, :] = (live_ref[...] * total).astype(out_ref.dtype)


def direct(wave, left_ops, right_ops, op_scales, sources, coupled, left_dims, right_dims):
    sectors, term_devices = lax.axis_size("sector"), lax.axis_size("term")
    chips = term_devices // 2
    rows, _, vectors, states = wave.shape
    terms, chosen = left_ops.shape[0], coupled.shape[1]
    bf16, f32 = jnp.bfloat16, jnp.float32

    any_spec, smem_spec = pl.BlockSpec(memory_space=pl.ANY), pl.BlockSpec(memory_space=SMEM)
    vmem_spec = pl.BlockSpec(memory_space=VMEM)
    hbm = lambda x: pltpu.with_memory_space_constraint(x, pltpu.HBM)
    shares = [swap(wave, "sector", sectors, m) for m in range(1, sectors)]
    ops, coops, scales, picks, mine, masks, live = pl.pallas_call(
        functools.partial(load_kernel, sectors),
        out_shape=(VMEM(left_ops.shape, bf16), VMEM(right_ops.shape, bf16), SMEM((terms,), f32),
                   SMEM((terms,), jnp.int32), VMEM((chosen, vectors, rows, states), f32),
                   VMEM((chosen, sectors, rows, states), f32), VMEM((rows, states), f32)),
        in_specs=[smem_spec] * 3 + [any_spec] * 5,
        out_specs=(vmem_spec, vmem_spec, smem_spec, smem_spec, vmem_spec, vmem_spec, vmem_spec),
        scratch_shapes=[VMEM(wave.shape, bf16), pltpu.SemaphoreType.DMA((5,))],
        compiler_params=pltpu.CompilerParams(vmem_limit_bytes=4 << 20),
    )(hbm(coupled), hbm(left_dims), hbm(right_dims), hbm(wave), hbm(left_ops), hbm(right_ops),
      hbm(op_scales.reshape(-1)), hbm(sources.reshape(-1)))
    own = call(pick_kernel, VMEM((chosen, vectors, rows, states), bf16), 0, 1 + sectors,
               (masks, mine, *shares))
    line = [own] + [swap(own, "term", term_devices, 2 * m) for m in range(1, chips)]
    line = line + [swap(b, "term", term_devices, 1) for b in line]
    send, keep = call(functools.partial(sigma_kernel, chips),
                      (VMEM((chips, vectors, rows, states), bf16), VMEM((chips, vectors, rows, states), f32)),
                      2, 2 + len(line),
                      (pltpu.with_memory_space_constraint(scales, SMEM), pltpu.with_memory_space_constraint(picks, SMEM), ops, coops, *line),
                      (VMEM((chosen, states, vectors * states), bf16),
                       VMEM((vectors * states, terms * states), bf16)))
    parts = call(functools.partial(split_kernel, chips),
                 (VMEM((vectors, rows, states), f32),)
                 + (VMEM((vectors, rows, states), bf16),) * (chips - 1),
                 0, 2, (keep, swap(send, "term", term_devices, 1)))
    others = [swap(parts[m], "term", term_devices, 2 * m) for m in range(1, chips)]
    return call(final_kernel, jax.ShapeDtypeStruct(wave.shape, bf16), 0, 1 + chips,
                (live, parts[0], *others))


def whole_kernel(scale_ref, source_ref, left_ref, right_ref, blocks_ref, out_ref, prod_ref):
    out_ref[...] = contract(scale_ref, source_ref, left_ref, right_ref, blocks_ref, prod_ref)


def gathered(wave, left_ops, right_ops, op_scales, sources, coupled, left_dims, right_dims):
    rows, _, vectors, states = wave.shape
    terms, chosen = left_ops.shape[0], coupled.shape[1]
    me, place = lax.axis_index("sector"), lax.axis_index("term")
    shares = lax.all_gather(wave[:, 0], "sector", axis=0)
    picks = coupled[0]
    row = lax.broadcasted_iota(jnp.int32, (1, rows, 1, states), 1) + place * rows
    col = lax.broadcasted_iota(jnp.int32, (1, rows, 1, states), 3)
    live = ((row < jnp.take(left_dims, picks)[:, None, None, None])
            & (col < jnp.take(right_dims, picks)[:, None, None, None]))
    own = jnp.where(live, jnp.take(shares, picks, axis=0), jnp.zeros((), wave.dtype))
    blocks = lax.all_gather(own, "term", axis=1, tiled=True).reshape(chosen, -1, vectors * states)
    total = call(whole_kernel, jax.ShapeDtypeStruct((vectors * states, states), jnp.float32),
                 2, 3, (op_scales.reshape(-1), sources.reshape(-1), left_ops, right_ops, blocks),
                 (VMEM((vectors * states, terms * states), jnp.bfloat16),))
    total = jnp.transpose(total.reshape(vectors, states, states), (1, 0, 2))
    row = lax.broadcasted_iota(jnp.int32, total.shape, 0)
    col = lax.broadcasted_iota(jnp.int32, total.shape, 2)
    total = jnp.where((row < left_dims[me]) & (col < right_dims[me]), total, 0.0)
    return lax.psum_scatter(total.astype(jnp.bfloat16), "term", scatter_dimension=0, tiled=True)[:, None]


def solution(mesh):
    in_specs = (
        P("term", "sector", None, None),
        P("term", "sector", None, None),
        P("term", "sector", None, None),
        P("term", "sector"),
        P("term", "sector"),
        P("sector", None),
        P(),
        P(),
    )
    out_specs = P("term", "sector", None, None)
    small = mesh.shape["sector"] == 4 and mesh.shape["term"] == 8
    return jax.shard_map(direct if small else gathered, mesh=mesh, in_specs=in_specs,
                         out_specs=out_specs, check_vma=False)
```

```python
import functools

import jax
import jax.numpy as jnp
from jax import lax
from jax.experimental import pallas as pl
from jax.experimental.pallas import tpu as pltpu
from jax.sharding import PartitionSpec as P

VMEM = pltpu.VMEM
SMEM = pltpu.SMEM


def swap(x, axis, size, mask):
    return lax.ppermute(x, axis, [(i, i ^ mask) for i in range(size)])


def load_kernel(sectors, coupled_ref, left_ref, right_ref, wave_ref, ops_ref, coops_ref, scale_ref, source_ref,
                ops_out, coops_out, scale_out, source_out, own_out, masks_out, live_out, wave_vmem, sems):
    copies = [pltpu.make_async_copy(src, dst, sems.at[n]) for n, (src, dst) in enumerate((
        (wave_ref, wave_vmem), (ops_ref, ops_out), (coops_ref, coops_out),
        (scale_ref, scale_out), (source_ref, source_out)))]
    for copy in copies:
        copy.start()
    chosen, vectors, rows, states = own_out.shape
    me, first_row = lax.axis_index("sector"), lax.axis_index("term") * rows
    row = lax.broadcasted_iota(jnp.int32, (rows, states), 0) + first_row
    col = lax.broadcasted_iota(jnp.int32, (rows, states), 1)
    live_out[...] = ((row < left_ref[me]) & (col < right_ref[me])).astype(jnp.float32)
    for c in range(chosen):
        sector = coupled_ref[0, c]
        live = ((row < left_ref[sector]) & (col < right_ref[sector])).astype(jnp.float32)
        for m in range(sectors):
            masks_out[c, m] = jnp.where((sector ^ me) == m, live, 0.0)
    copies[0].wait()
    for v in range(vectors):
        value = wave_vmem[:, 0, v, :].astype(jnp.float32)
        for c in range(chosen):
            own_out[c, v] = masks_out[c, 0] * value
    for copy in copies[1:]:
        copy.wait()


def pick_kernel(masks_ref, own_ref, *refs):
    blocks, out_ref = refs[:-1], refs[-1]
    chosen, vectors = out_ref.shape[:2]
    for v in range(vectors):
        values = [block[:, 0, v, :].astype(jnp.float32) for block in blocks]
        for c in range(chosen):
            total = own_ref[c, v]
            for m, value in enumerate(values):
                total = total + masks_ref[c, m + 1] * value
            out_ref[c, v] = total.astype(out_ref.dtype)


def contract(scale_ref, source_ref, left_ref, right_ref, psi_ref, prod_ref):
    terms, _, states, _ = left_ref.shape
    vectors = psi_ref.shape[2] // states
    for t in range(terms):
        prod = jnp.dot(left_ref[t, 0], psi_ref[source_ref[t]], preferred_element_type=jnp.float32)
        prod = (prod * scale_ref[t]).astype(jnp.bfloat16)
        for v in range(vectors):
            prod_ref[v * states:(v + 1) * states, t * states:(t + 1) * states] = (
                prod[:, v * states:(v + 1) * states])
    return jnp.dot(prod_ref[...], right_ref[...].reshape(terms * states, states),
                   preferred_element_type=jnp.float32)


def project(coops_ref, scale_ref, source_ref, blocks, core, stack_ref, prod_ref):
    chosen, vectors, rows, states = blocks[0].shape
    chip = lax.axis_index("term") >> 1
    starts = []
    for n, block in enumerate(blocks):
        starts.append(pl.multiple_of(((chip ^ n) * 2 + core) * rows, rows))
        for c in range(chosen):
            for v in range(vectors):
                at = (n * vectors + v) * rows
                stack_ref[c, at:at + rows] = block[c, v]
    for t in range(coops_ref.shape[0]):
        prod = jnp.dot(stack_ref[source_ref[t]], coops_ref[t, 0], preferred_element_type=jnp.float32)
        prod = (prod * scale_ref[t]).astype(prod_ref.dtype)
        for n, start in enumerate(starts):
            for v in range(vectors):
                at = (n * vectors + v) * rows
                prod_ref[t, pl.ds(start, rows), v * states:(v + 1) * states] = prod[at:at + rows]


def apply_left(ops_ref, prod_ref, core, out_ref):
    chips, vectors, rows, states = out_ref.shape
    total = None
    for t in range(ops_ref.shape[0]):
        left = jnp.concatenate(
            [ops_ref[t, 0, pl.ds(pl.multiple_of((2 * z + core) * rows, rows), rows), :] for z in range(chips)])
        part = jnp.dot(left, prod_ref[t], preferred_element_type=jnp.float32)
        total = part if total is None else total + part
    for z in range(chips):
        for v in range(vectors):
            out_ref[z, v] = total[z * rows:(z + 1) * rows, v * states:(v + 1) * states].astype(out_ref.dtype)


def first_kernel(scale_ref, source_ref, coops_ref, *refs):
    blocks, prod_ref, stack_ref = refs[:-2], refs[-2], refs[-1]
    project(coops_ref, scale_ref, source_ref, blocks, lax.axis_index("term") & 1, stack_ref, prod_ref)


def second_kernel(scale_ref, source_ref, coops_ref, ops_ref, prod_in, *refs):
    blocks, prod_ref, send_ref, stack_ref = refs[:-3], refs[-3], refs[-2], refs[-1]
    other = 1 - (lax.axis_index("term") & 1)
    project(coops_ref, scale_ref, source_ref, blocks, other, stack_ref, prod_ref)
    apply_left(ops_ref, prod_ref, other, send_ref)


def third_kernel(ops_ref, prod_ref, keep_ref):
    apply_left(ops_ref, prod_ref, lax.axis_index("term") & 1, keep_ref)


def split_kernel(chips, keep_ref, recv_ref, *outs):
    chip = lax.axis_index("term") >> 1
    for n in range(chips):
        at = chip ^ n
        outs[n][...] = (keep_ref[at] + recv_ref[at].astype(jnp.float32)).astype(outs[n].dtype)


def call(kernel, outs, smem, vmem, args, scratch=(), aliases={}):
    args = [pltpu.with_memory_space_constraint(x, SMEM if n < smem else VMEM) for n, x in enumerate(args)]
    return pl.pallas_call(
        kernel,
        out_shape=outs,
        in_specs=[pl.BlockSpec(memory_space=SMEM)] * smem + [pl.BlockSpec(memory_space=VMEM)] * vmem,
        out_specs=jax.tree.map(lambda _: pl.BlockSpec(memory_space=VMEM), outs),
        scratch_shapes=list(scratch),
        input_output_aliases=aliases,
        compiler_params=pltpu.CompilerParams(vmem_limit_bytes=24 << 20),
    )(*args)


def final_kernel(live_ref, total_ref, *refs):
    parts, out_ref = refs[:-1], refs[-1]
    for v in range(total_ref.shape[0]):
        total = total_ref[v]
        for part in parts:
            total = total + part[v].astype(jnp.float32)
        out_ref[:, 0, v, :] = (live_ref[...] * total).astype(out_ref.dtype)


def direct(wave, left_ops, right_ops, op_scales, sources, coupled, left_dims, right_dims):
    sectors, term_devices = lax.axis_size("sector"), lax.axis_size("term")
    chips = term_devices // 2
    rows, _, vectors, states = wave.shape
    terms, chosen = left_ops.shape[0], coupled.shape[1]
    bf16, f32 = jnp.bfloat16, jnp.float32

    any_spec, smem_spec = pl.BlockSpec(memory_space=pl.ANY), pl.BlockSpec(memory_space=SMEM)
    vmem_spec = pl.BlockSpec(memory_space=VMEM)
    hbm = lambda x: pltpu.with_memory_space_constraint(x, pltpu.HBM)
    shares = [swap(wave, "sector", sectors, m) for m in range(1, sectors)]
    ops, coops, scales, picks, mine, masks, live = pl.pallas_call(
        functools.partial(load_kernel, sectors),
        out_shape=(VMEM(left_ops.shape, bf16), VMEM(right_ops.shape, bf16), SMEM((terms,), f32),
                   SMEM((terms,), jnp.int32), VMEM((chosen, vectors, rows, states), f32),
                   VMEM((chosen, sectors, rows, states), f32), VMEM((rows, states), f32)),
        in_specs=[smem_spec] * 3 + [any_spec] * 5,
        out_specs=(vmem_spec, vmem_spec, smem_spec, smem_spec, vmem_spec, vmem_spec, vmem_spec),
        scratch_shapes=[VMEM(wave.shape, bf16), pltpu.SemaphoreType.DMA((5,))],
        compiler_params=pltpu.CompilerParams(vmem_limit_bytes=4 << 20),
    )(hbm(coupled), hbm(left_dims), hbm(right_dims), hbm(wave), hbm(left_ops), hbm(right_ops),
      hbm(op_scales.reshape(-1)), hbm(sources.reshape(-1)))
    own = call(pick_kernel, VMEM((chosen, vectors, rows, states), bf16), 0, 1 + sectors,
               (masks, mine, *shares))
    line = [own] + [swap(own, "term", term_devices, 2 * m) for m in range(1, chips)]
    pair = [swap(b, "term", term_devices, 1) for b in line]
    stack = VMEM((chosen, chips * vectors * rows, states), bf16)
    prod_shape = VMEM((terms, states, vectors * states), bf16)
    piece = (chips, vectors, rows, states)
    prod = call(first_kernel, prod_shape, 2, 1 + chips, (scales, picks, coops, *line), (stack,))
    prod, send = call(second_kernel, (prod_shape, VMEM(piece, bf16)), 2, 3 + chips,
                      (scales, picks, coops, ops, prod, *pair), (stack,), {4: 0})
    keep = call(third_kernel, VMEM(piece, f32), 0, 2, (ops, prod))
    parts = call(functools.partial(split_kernel, chips),
                 (VMEM((vectors, rows, states), f32),)
                 + (VMEM((vectors, rows, states), bf16),) * (chips - 1),
                 0, 2, (keep, swap(send, "term", term_devices, 1)))
    others = [swap(parts[m], "term", term_devices, 2 * m) for m in range(chips - 1, 0, -1)]
    return call(final_kernel, jax.ShapeDtypeStruct(wave.shape, bf16), 0, 1 + chips,
                (live, parts[0], *others))


def whole_kernel(scale_ref, source_ref, left_ref, right_ref, blocks_ref, out_ref, prod_ref):
    out_ref[...] = contract(scale_ref, source_ref, left_ref, right_ref, blocks_ref, prod_ref)


def gathered(wave, left_ops, right_ops, op_scales, sources, coupled, left_dims, right_dims):
    rows, _, vectors, states = wave.shape
    terms, chosen = left_ops.shape[0], coupled.shape[1]
    me, place = lax.axis_index("sector"), lax.axis_index("term")
    shares = lax.all_gather(wave[:, 0], "sector", axis=0)
    picks = coupled[0]
    row = lax.broadcasted_iota(jnp.int32, (1, rows, 1, states), 1) + place * rows
    col = lax.broadcasted_iota(jnp.int32, (1, rows, 1, states), 3)
    live = ((row < jnp.take(left_dims, picks)[:, None, None, None])
            & (col < jnp.take(right_dims, picks)[:, None, None, None]))
    own = jnp.where(live, jnp.take(shares, picks, axis=0), jnp.zeros((), wave.dtype))
    blocks = lax.all_gather(own, "term", axis=1, tiled=True).reshape(chosen, -1, vectors * states)
    total = call(whole_kernel, jax.ShapeDtypeStruct((vectors * states, states), jnp.float32),
                 2, 3, (op_scales.reshape(-1), sources.reshape(-1), left_ops, right_ops, blocks),
                 (VMEM((vectors * states, terms * states), jnp.bfloat16),))
    total = jnp.transpose(total.reshape(vectors, states, states), (1, 0, 2))
    row = lax.broadcasted_iota(jnp.int32, total.shape, 0)
    col = lax.broadcasted_iota(jnp.int32, total.shape, 2)
    total = jnp.where((row < left_dims[me]) & (col < right_dims[me]), total, 0.0)
    return lax.psum_scatter(total.astype(jnp.bfloat16), "term", scatter_dimension=0, tiled=True)[:, None]


def solution(mesh):
    in_specs = (
        P("term", "sector", None, None),
        P("term", "sector", None, None),
        P("term", "sector", None, None),
        P("term", "sector"),
        P("term", "sector"),
        P("sector", None),
        P(),
        P(),
    )
    out_specs = P("term", "sector", None, None)
    small = mesh.shape["sector"] == 4 and mesh.shape["term"] == 8
    return jax.shard_map(direct if small else gathered, mesh=mesh, in_specs=in_specs,
                         out_specs=out_specs, check_vma=False)
```

```python
import functools

import jax
import jax.numpy as jnp
from jax import lax
from jax.experimental import pallas as pl
from jax.experimental.pallas import tpu as pltpu
from jax.sharding import PartitionSpec as P


VMEM = pltpu.VMEM
SMEM = pltpu.SMEM
GROUPS = (((0, 0), (0, 1)), ((1, 0), (2, 0), (3, 0), (3, 1)), ((1, 1), (2, 1)))


def swap(x, axis, size, mask):
    return lax.ppermute(x, axis, [(i, i ^ mask) for i in range(size)])


def along(x, size, by):
    pairs = [(i, (i + 2 * by) % size) for i in range(size)]
    return lax.ppermute(x, "term", pairs)


def load_kernel(sectors, coupled_ref, left_ref, right_ref, wave_ref, ops_ref, coops_ref, scale_ref, source_ref,
                ops_out, coops_out, scale_out, source_out, own_out, masks_out, live_out, wave_vmem, sems):
    copies = [pltpu.make_async_copy(src, dst, sems.at[n]) for n, (src, dst) in enumerate((
        (wave_ref, wave_vmem), (ops_ref, ops_out), (coops_ref, coops_out),
        (scale_ref, scale_out), (source_ref, source_out)))]
    for copy in copies:
        copy.start()
    chosen, vectors, rows, states = own_out.shape
    me, first_row = lax.axis_index("sector"), lax.axis_index("term") * rows
    row = lax.broadcasted_iota(jnp.int32, (rows, states), 0) + first_row
    col = lax.broadcasted_iota(jnp.int32, (rows, states), 1)
    live_out[...] = ((row < left_ref[me]) & (col < right_ref[me])).astype(jnp.float32)
    for c in range(chosen):
        sector = coupled_ref[0, c]
        live = ((row < left_ref[sector]) & (col < right_ref[sector])).astype(jnp.float32)
        for m in range(sectors):
            masks_out[c, m] = jnp.where((sector ^ me) == m, live, 0.0)
    copies[0].wait()
    for v in range(vectors):
        value = wave_vmem[:, 0, v, :].astype(jnp.float32)
        for c in range(chosen):
            own_out[c, v] = masks_out[c, 0] * value
    for copy in copies[1:]:
        copy.wait()


def pick_kernel(masks_ref, own_ref, *refs):
    blocks, out_ref = refs[:-1], refs[-1]
    chosen, vectors = out_ref.shape[:2]
    for v in range(vectors):
        values = [block[:, 0, v, :].astype(jnp.float32) for block in blocks]
        for c in range(chosen):
            total = own_ref[c, v]
            for m, value in enumerate(values):
                total = total + masks_ref[c, m + 1] * value
            out_ref[c, v] = total.astype(out_ref.dtype)


def contract(scale_ref, source_ref, left_ref, right_ref, psi_ref, prod_ref):
    terms, _, states, _ = left_ref.shape
    vectors = psi_ref.shape[2] // states
    for t in range(terms):
        prod = jnp.dot(left_ref[t, 0], psi_ref[source_ref[t]], preferred_element_type=jnp.float32)
        prod = (prod * scale_ref[t]).astype(jnp.bfloat16)
        for v in range(vectors):
            prod_ref[v * states:(v + 1) * states, t * states:(t + 1) * states] = (
                prod[:, v * states:(v + 1) * states])
    return jnp.dot(prod_ref[...], right_ref[...].reshape(terms * states, states),
                   preferred_element_type=jnp.float32)


def project(coops_ref, scale_ref, source_ref, blocks, places, stack_ref, prod_ref):
    chosen, vectors, rows, states = blocks[0].shape
    for n, block in enumerate(blocks):
        for c in range(chosen):
            for v in range(vectors):
                at = (n * vectors + v) * rows
                stack_ref[c, at:at + rows] = block[c, v]
    used = len(blocks) * vectors * rows
    for t in range(coops_ref.shape[0]):
        prod = jnp.dot(stack_ref[source_ref[t], :used], coops_ref[t, 0], preferred_element_type=jnp.float32)
        prod = (prod * scale_ref[t]).astype(prod_ref.dtype)
        for n, place in enumerate(places):
            start = pl.multiple_of(place * rows, rows)
            for v in range(vectors):
                at = (n * vectors + v) * rows
                prod_ref[t, pl.ds(start, rows), v * states:(v + 1) * states] = prod[at:at + rows]


def owners(kinds):
    return [lax.axis_index("term") ^ (2 * away + other) for away, other in kinds]


def apply_left(ops_ref, prod_ref, core, out_ref):
    chips, vectors, rows, states = out_ref.shape
    total = None
    for t in range(ops_ref.shape[0]):
        left = jnp.concatenate(
            [ops_ref[t, 0, pl.ds(pl.multiple_of((2 * z + core) * rows, rows), rows), :] for z in range(chips)])
        part = jnp.dot(left, prod_ref[t], preferred_element_type=jnp.float32)
        total = part if total is None else total + part
    for z in range(chips):
        for v in range(vectors):
            out_ref[z, v] = total[z * rows:(z + 1) * rows, v * states:(v + 1) * states].astype(out_ref.dtype)


def first_kernel(kinds, scale_ref, source_ref, coops_ref, *refs):
    blocks, prod_ref, stack_ref = refs[:-2], refs[-2], refs[-1]
    project(coops_ref, scale_ref, source_ref, blocks, owners(kinds), stack_ref, prod_ref)


def more_kernel(kinds, scale_ref, source_ref, coops_ref, prod_in, *refs):
    blocks, prod_ref, stack_ref = refs[:-2], refs[-2], refs[-1]
    project(coops_ref, scale_ref, source_ref, blocks, owners(kinds), stack_ref, prod_ref)


def second_kernel(kinds, scale_ref, source_ref, coops_ref, ops_ref, prod_in, *refs):
    blocks, prod_ref, send_ref, stack_ref = refs[:-3], refs[-3], refs[-2], refs[-1]
    project(coops_ref, scale_ref, source_ref, blocks, owners(kinds), stack_ref, prod_ref)
    apply_left(ops_ref, prod_ref, 1 - (lax.axis_index("term") & 1), send_ref)


def third_kernel(ops_ref, prod_ref, keep_ref):
    apply_left(ops_ref, prod_ref, lax.axis_index("term") & 1, keep_ref)


def split_kernel(chips, keep_ref, recv_ref, *outs):
    chip = lax.axis_index("term") >> 1
    for n in range(chips):
        at = lax.rem(chip + n, chips)
        outs[n][...] = (keep_ref[at] + recv_ref[at].astype(jnp.float32)).astype(outs[n].dtype)


def call(kernel, outs, smem, vmem, args, scratch=(), aliases={}):
    args = [pltpu.with_memory_space_constraint(x, SMEM if n < smem else VMEM) for n, x in enumerate(args)]
    return pl.pallas_call(
        kernel,
        out_shape=outs,
        in_specs=[pl.BlockSpec(memory_space=SMEM)] * smem + [pl.BlockSpec(memory_space=VMEM)] * vmem,
        out_specs=jax.tree.map(lambda _: pl.BlockSpec(memory_space=VMEM), outs),
        scratch_shapes=list(scratch),
        input_output_aliases=aliases,
        compiler_params=pltpu.CompilerParams(vmem_limit_bytes=24 << 20),
    )(*args)


def final_kernel(live_ref, total_ref, *refs):
    parts, out_ref = refs[:-1], refs[-1]
    for v in range(total_ref.shape[0]):
        total = total_ref[v]
        for part in parts:
            total = total + part[v].astype(jnp.float32)
        out_ref[:, 0, v, :] = (live_ref[...] * total).astype(out_ref.dtype)


def direct(wave, left_ops, right_ops, op_scales, sources, coupled, left_dims, right_dims):
    sectors, term_devices = lax.axis_size("sector"), lax.axis_size("term")
    chips = term_devices // 2
    rows, _, vectors, states = wave.shape
    terms, chosen = left_ops.shape[0], coupled.shape[1]
    bf16, f32 = jnp.bfloat16, jnp.float32

    any_spec, smem_spec = pl.BlockSpec(memory_space=pl.ANY), pl.BlockSpec(memory_space=SMEM)
    vmem_spec = pl.BlockSpec(memory_space=VMEM)
    hbm = lambda x: pltpu.with_memory_space_constraint(x, pltpu.HBM)
    shares = [swap(wave, "sector", sectors, m) for m in range(1, sectors)]
    ops, coops, scales, picks, mine, masks, live = pl.pallas_call(
        functools.partial(load_kernel, sectors),
        out_shape=(VMEM(left_ops.shape, bf16), VMEM(right_ops.shape, bf16), SMEM((terms,), f32),
                   SMEM((terms,), jnp.int32), VMEM((chosen, vectors, rows, states), f32),
                   VMEM((chosen, sectors, rows, states), f32), VMEM((rows, states), f32)),
        in_specs=[smem_spec] * 3 + [any_spec] * 5,
        out_specs=(vmem_spec, vmem_spec, smem_spec, smem_spec, vmem_spec, vmem_spec, vmem_spec),
        scratch_shapes=[VMEM(wave.shape, bf16), pltpu.SemaphoreType.DMA((5,))],
        compiler_params=pltpu.CompilerParams(vmem_limit_bytes=4 << 20),
    )(hbm(coupled), hbm(left_dims), hbm(right_dims), hbm(wave), hbm(left_ops), hbm(right_ops),
      hbm(op_scales.reshape(-1)), hbm(sources.reshape(-1)))
    own = call(pick_kernel, VMEM((chosen, vectors, rows, states), bf16), 0, 1 + sectors,
               (masks, mine, *shares))
    line = [own] + [swap(own, "term", term_devices, 2 * m) for m in range(1, chips)]
    pair = [swap(b, "term", term_devices, 1) for b in line]
    prod_shape = VMEM((terms, states, vectors * states), bf16)
    piece = (chips, vectors, rows, states)
    blocks = {(n, o): (pair if o else line)[n] for n in range(chips) for o in range(2)}
    stack = lambda kinds: (VMEM((chosen, len(kinds) * vectors * rows, states), bf16),)
    prod = None
    for kinds in GROUPS[:-1]:
        given = [blocks[kind] for kind in kinds]
        if prod is None:
            prod = call(functools.partial(first_kernel, kinds), prod_shape, 2, 1 + len(kinds),
                        (scales, picks, coops, *given), stack(kinds))
        else:
            prod = call(functools.partial(more_kernel, kinds), prod_shape, 2, 2 + len(kinds),
                        (scales, picks, coops, prod, *given), stack(kinds), {3: 0})
    kinds = GROUPS[-1]
    prod, send = call(functools.partial(second_kernel, kinds), (prod_shape, VMEM(piece, bf16)), 2, 3 + len(kinds),
                      (scales, picks, coops, ops, prod, *[blocks[kind] for kind in kinds]), stack(kinds), {4: 0})
    keep = call(third_kernel, VMEM(piece, f32), 0, 2, (ops, prod))
    parts = call(functools.partial(split_kernel, chips),
                 (VMEM((vectors, rows, states), f32),)
                 + (VMEM((vectors, rows, states), bf16),) * (chips - 1),
                 0, 2, (keep, swap(send, "term", term_devices, 1)))
    others = [along(parts[m], term_devices, m) for m in range(1, chips)]
    return call(final_kernel, jax.ShapeDtypeStruct(wave.shape, bf16), 0, 1 + chips,
                (live, parts[0], *others))


def whole_kernel(scale_ref, source_ref, left_ref, right_ref, blocks_ref, out_ref, prod_ref):
    out_ref[...] = contract(scale_ref, source_ref, left_ref, right_ref, blocks_ref, prod_ref)


def gathered(wave, left_ops, right_ops, op_scales, sources, coupled, left_dims, right_dims):
    rows, _, vectors, states = wave.shape
    terms, chosen = left_ops.shape[0], coupled.shape[1]
    me, place = lax.axis_index("sector"), lax.axis_index("term")
    shares = lax.all_gather(wave[:, 0], "sector", axis=0)
    picks = coupled[0]
    row = lax.broadcasted_iota(jnp.int32, (1, rows, 1, states), 1) + place * rows
    col = lax.broadcasted_iota(jnp.int32, (1, rows, 1, states), 3)
    live = ((row < jnp.take(left_dims, picks)[:, None, None, None])
            & (col < jnp.take(right_dims, picks)[:, None, None, None]))
    own = jnp.where(live, jnp.take(shares, picks, axis=0), jnp.zeros((), wave.dtype))
    blocks = lax.all_gather(own, "term", axis=1, tiled=True).reshape(chosen, -1, vectors * states)
    total = call(whole_kernel, jax.ShapeDtypeStruct((vectors * states, states), jnp.float32),
                 2, 3, (op_scales.reshape(-1), sources.reshape(-1), left_ops, right_ops, blocks),
                 (VMEM((vectors * states, terms * states), jnp.bfloat16),))
    total = jnp.transpose(total.reshape(vectors, states, states), (1, 0, 2))
    row = lax.broadcasted_iota(jnp.int32, total.shape, 0)
    col = lax.broadcasted_iota(jnp.int32, total.shape, 2)
    total = jnp.where((row < left_dims[me]) & (col < right_dims[me]), total, 0.0)
    return lax.psum_scatter(total.astype(jnp.bfloat16), "term", scatter_dimension=0, tiled=True)[:, None]


def solution(mesh):
    in_specs = (
        P("term", "sector", None, None),
        P("term", "sector", None, None),
        P("term", "sector", None, None),
        P("term", "sector"),
        P("term", "sector"),
        P("sector", None),
        P(),
        P(),
    )
    out_specs = P("term", "sector", None, None)
    small = mesh.shape["sector"] == 4 and mesh.shape["term"] == 8

    def local(*args):
        return (direct if small else gathered)(*args)

    return jax.shard_map(local, mesh=mesh, in_specs=in_specs, out_specs=out_specs, check_vma=False)
```

```python
import functools

import jax
import jax.numpy as jnp
from jax import lax
from jax.experimental import pallas as pl
from jax.experimental.pallas import tpu as pltpu
from jax.sharding import PartitionSpec as P


VMEM = pltpu.VMEM
SMEM = pltpu.SMEM
GROUPS = (((0, 0), (0, 1)), ((1, 0), (2, 0), (3, 0), (3, 1)), ((1, 1), (2, 1)))


def swap(x, axis, size, mask):
    return lax.ppermute(x, axis, [(i, i ^ mask) for i in range(size)])


def along(x, size, by):
    pairs = [(i, (i + 2 * by) % size) for i in range(size)]
    return lax.ppermute(x, "term", pairs)


def load_kernel(sectors, coupled_ref, left_ref, right_ref, wave_ref, ops_ref, coops_ref, scale_ref, source_ref,
                ops_out, coops_out, scale_out, source_out, own_out, masks_out, live_out, wave_vmem, sems):
    copies = [pltpu.make_async_copy(src, dst, sems.at[n]) for n, (src, dst) in enumerate((
        (wave_ref, wave_vmem), (ops_ref, ops_out), (coops_ref, coops_out),
        (scale_ref, scale_out), (source_ref, source_out)))]
    for copy in copies:
        copy.start()
    chosen, vectors, rows, states = own_out.shape
    me, first_row = lax.axis_index("sector"), lax.axis_index("term") * rows
    row = lax.broadcasted_iota(jnp.int32, (rows, states), 0) + first_row
    col = lax.broadcasted_iota(jnp.int32, (rows, states), 1)
    live_out[...] = ((row < left_ref[me]) & (col < right_ref[me])).astype(jnp.float32)
    for c in range(chosen):
        sector = coupled_ref[0, c]
        live = ((row < left_ref[sector]) & (col < right_ref[sector])).astype(jnp.float32)
        for m in range(sectors):
            masks_out[c, m] = jnp.where((sector ^ me) == m, live, 0.0)
    copies[0].wait()
    for v in range(vectors):
        value = wave_vmem[:, 0, v, :].astype(jnp.float32)
        for c in range(chosen):
            own_out[c, v] = masks_out[c, 0] * value
    for copy in copies[1:]:
        copy.wait()


def pick_kernel(masks_ref, own_ref, *refs):
    blocks, out_ref = refs[:-1], refs[-1]
    chosen, vectors = out_ref.shape[:2]
    for v in range(vectors):
        values = [block[:, 0, v, :].astype(jnp.float32) for block in blocks]
        for c in range(chosen):
            total = own_ref[c, v]
            for m, value in enumerate(values):
                total = total + masks_ref[c, m + 1] * value
            out_ref[c, v] = total.astype(out_ref.dtype)


def contract(scale_ref, source_ref, left_ref, right_ref, psi_ref, prod_ref):
    terms, _, states, _ = left_ref.shape
    vectors = psi_ref.shape[2] // states
    for t in range(terms):
        prod = jnp.dot(left_ref[t, 0], psi_ref[source_ref[t]], preferred_element_type=jnp.float32)
        prod = (prod * scale_ref[t]).astype(jnp.bfloat16)
        for v in range(vectors):
            prod_ref[v * states:(v + 1) * states, t * states:(t + 1) * states] = (
                prod[:, v * states:(v + 1) * states])
    return jnp.dot(prod_ref[...], right_ref[...].reshape(terms * states, states),
                   preferred_element_type=jnp.float32)


def project(coops_ref, scale_ref, source_ref, blocks, places, stack_ref, prod_ref):
    chosen, vectors, rows, states = blocks[0].shape
    for n, block in enumerate(blocks):
        for c in range(chosen):
            for v in range(vectors):
                at = (n * vectors + v) * rows
                stack_ref[c, at:at + rows] = block[c, v]
    used = len(blocks) * vectors * rows
    for t in range(coops_ref.shape[0]):
        prod = jnp.dot(stack_ref[source_ref[t], :used], coops_ref[t, 0], preferred_element_type=jnp.float32)
        prod = (prod * scale_ref[t]).astype(prod_ref.dtype)
        for n, place in enumerate(places):
            start = pl.multiple_of(place * rows, rows)
            for v in range(vectors):
                at = (n * vectors + v) * rows
                prod_ref[t, pl.ds(start, rows), v * states:(v + 1) * states] = prod[at:at + rows]


def owners(kinds):
    return [lax.axis_index("term") ^ (2 * away + other) for away, other in kinds]


def apply_left(ops_ref, prod_ref, core, out_ref):
    chips, vectors, rows, states = out_ref.shape
    terms, states, width = prod_ref.shape
    starts = [pl.multiple_of((2 * z + core) * rows, rows) for z in range(chips)]
    left = jnp.concatenate([jnp.concatenate([ops_ref[t, 0, pl.ds(start, rows), :] for t in range(terms)], axis=1)
                            for start in starts])
    total = jnp.dot(left, prod_ref[...].reshape(terms * states, width), preferred_element_type=jnp.float32)
    for z in range(chips):
        for v in range(vectors):
            out_ref[z, v] = total[z * rows:(z + 1) * rows, v * states:(v + 1) * states].astype(out_ref.dtype)


def first_kernel(kinds, scale_ref, source_ref, coops_ref, *refs):
    blocks, prod_ref, stack_ref = refs[:-2], refs[-2], refs[-1]
    project(coops_ref, scale_ref, source_ref, blocks, owners(kinds), stack_ref, prod_ref)


def more_kernel(kinds, scale_ref, source_ref, coops_ref, prod_in, *refs):
    blocks, prod_ref, stack_ref = refs[:-2], refs[-2], refs[-1]
    project(coops_ref, scale_ref, source_ref, blocks, owners(kinds), stack_ref, prod_ref)


def second_kernel(kinds, scale_ref, source_ref, coops_ref, ops_ref, prod_in, *refs):
    blocks, prod_ref, send_ref, stack_ref = refs[:-3], refs[-3], refs[-2], refs[-1]
    project(coops_ref, scale_ref, source_ref, blocks, owners(kinds), stack_ref, prod_ref)
    apply_left(ops_ref, prod_ref, 1 - (lax.axis_index("term") & 1), send_ref)


def third_kernel(ops_ref, prod_ref, keep_ref):
    apply_left(ops_ref, prod_ref, lax.axis_index("term") & 1, keep_ref)


def split_kernel(chips, keep_ref, recv_ref, *outs):
    chip = lax.axis_index("term") >> 1
    for n in range(chips):
        at = lax.rem(chip + n, chips)
        outs[n][...] = (keep_ref[at] + recv_ref[at].astype(jnp.float32)).astype(outs[n].dtype)


def call(kernel, outs, smem, vmem, args, scratch=(), aliases={}):
    args = [pltpu.with_memory_space_constraint(x, SMEM if n < smem else VMEM) for n, x in enumerate(args)]
    return pl.pallas_call(
        kernel,
        out_shape=outs,
        in_specs=[pl.BlockSpec(memory_space=SMEM)] * smem + [pl.BlockSpec(memory_space=VMEM)] * vmem,
        out_specs=jax.tree.map(lambda _: pl.BlockSpec(memory_space=VMEM), outs),
        scratch_shapes=list(scratch),
        input_output_aliases=aliases,
        compiler_params=pltpu.CompilerParams(vmem_limit_bytes=24 << 20),
    )(*args)


def final_kernel(live_ref, total_ref, *refs):
    parts, out_ref = refs[:-1], refs[-1]
    for v in range(total_ref.shape[0]):
        total = total_ref[v]
        for part in parts:
            total = total + part[v].astype(jnp.float32)
        out_ref[:, 0, v, :] = (live_ref[...] * total).astype(out_ref.dtype)


def direct(wave, left_ops, right_ops, op_scales, sources, coupled, left_dims, right_dims):
    sectors, term_devices = lax.axis_size("sector"), lax.axis_size("term")
    chips = term_devices // 2
    rows, _, vectors, states = wave.shape
    terms, chosen = left_ops.shape[0], coupled.shape[1]
    bf16, f32 = jnp.bfloat16, jnp.float32

    any_spec, smem_spec = pl.BlockSpec(memory_space=pl.ANY), pl.BlockSpec(memory_space=SMEM)
    vmem_spec = pl.BlockSpec(memory_space=VMEM)
    hbm = lambda x: pltpu.with_memory_space_constraint(x, pltpu.HBM)
    shares = [swap(wave, "sector", sectors, m) for m in range(1, sectors)]
    ops, coops, scales, picks, mine, masks, live = pl.pallas_call(
        functools.partial(load_kernel, sectors),
        out_shape=(VMEM(left_ops.shape, bf16), VMEM(right_ops.shape, bf16), SMEM((terms,), f32),
                   SMEM((terms,), jnp.int32), VMEM((chosen, vectors, rows, states), f32),
                   VMEM((chosen, sectors, rows, states), f32), VMEM((rows, states), f32)),
        in_specs=[smem_spec] * 3 + [any_spec] * 5,
        out_specs=(vmem_spec, vmem_spec, smem_spec, smem_spec, vmem_spec, vmem_spec, vmem_spec),
        scratch_shapes=[VMEM(wave.shape, bf16), pltpu.SemaphoreType.DMA((5,))],
        compiler_params=pltpu.CompilerParams(vmem_limit_bytes=4 << 20),
    )(hbm(coupled), hbm(left_dims), hbm(right_dims), hbm(wave), hbm(left_ops), hbm(right_ops),
      hbm(op_scales.reshape(-1)), hbm(sources.reshape(-1)))
    own = call(pick_kernel, VMEM((chosen, vectors, rows, states), bf16), 0, 1 + sectors,
               (masks, mine, *shares))
    line = [own] + [swap(own, "term", term_devices, 2 * m) for m in range(1, chips)]
    pair = [swap(b, "term", term_devices, 1) for b in line]
    prod_shape = VMEM((terms, states, vectors * states), bf16)
    piece = (chips, vectors, rows, states)
    blocks = {(n, o): (pair if o else line)[n] for n in range(chips) for o in range(2)}
    stack = lambda kinds: (VMEM((chosen, len(kinds) * vectors * rows, states), bf16),)
    prod = None
    for kinds in GROUPS[:-1]:
        given = [blocks[kind] for kind in kinds]
        if prod is None:
            prod = call(functools.partial(first_kernel, kinds), prod_shape, 2, 1 + len(kinds),
                        (scales, picks, coops, *given), stack(kinds))
        else:
            prod = call(functools.partial(more_kernel, kinds), prod_shape, 2, 2 + len(kinds),
                        (scales, picks, coops, prod, *given), stack(kinds), {3: 0})
    kinds = GROUPS[-1]
    prod, send = call(functools.partial(second_kernel, kinds), (prod_shape, VMEM(piece, bf16)), 2, 3 + len(kinds),
                      (scales, picks, coops, ops, prod, *[blocks[kind] for kind in kinds]), stack(kinds), {4: 0})
    keep = call(third_kernel, VMEM(piece, f32), 0, 2, (ops, prod))
    parts = call(functools.partial(split_kernel, chips),
                 (VMEM((vectors, rows, states), f32),)
                 + (VMEM((vectors, rows, states), bf16),) * (chips - 1),
                 0, 2, (keep, swap(send, "term", term_devices, 1)))
    others = [along(parts[m], term_devices, m) for m in range(1, chips)]
    return call(final_kernel, jax.ShapeDtypeStruct(wave.shape, bf16), 0, 1 + chips,
                (live, parts[0], *others))


def whole_kernel(scale_ref, source_ref, left_ref, right_ref, blocks_ref, out_ref, prod_ref):
    out_ref[...] = contract(scale_ref, source_ref, left_ref, right_ref, blocks_ref, prod_ref)


def gathered(wave, left_ops, right_ops, op_scales, sources, coupled, left_dims, right_dims):
    rows, _, vectors, states = wave.shape
    terms, chosen = left_ops.shape[0], coupled.shape[1]
    me, place = lax.axis_index("sector"), lax.axis_index("term")
    shares = lax.all_gather(wave[:, 0], "sector", axis=0)
    picks = coupled[0]
    row = lax.broadcasted_iota(jnp.int32, (1, rows, 1, states), 1) + place * rows
    col = lax.broadcasted_iota(jnp.int32, (1, rows, 1, states), 3)
    live = ((row < jnp.take(left_dims, picks)[:, None, None, None])
            & (col < jnp.take(right_dims, picks)[:, None, None, None]))
    own = jnp.where(live, jnp.take(shares, picks, axis=0), jnp.zeros((), wave.dtype))
    blocks = lax.all_gather(own, "term", axis=1, tiled=True).reshape(chosen, -1, vectors * states)
    total = call(whole_kernel, jax.ShapeDtypeStruct((vectors * states, states), jnp.float32),
                 2, 3, (op_scales.reshape(-1), sources.reshape(-1), left_ops, right_ops, blocks),
                 (VMEM((vectors * states, terms * states), jnp.bfloat16),))
    total = jnp.transpose(total.reshape(vectors, states, states), (1, 0, 2))
    row = lax.broadcasted_iota(jnp.int32, total.shape, 0)
    col = lax.broadcasted_iota(jnp.int32, total.shape, 2)
    total = jnp.where((row < left_dims[me]) & (col < right_dims[me]), total, 0.0)
    return lax.psum_scatter(total.astype(jnp.bfloat16), "term", scatter_dimension=0, tiled=True)[:, None]


def solution(mesh):
    in_specs = (
        P("term", "sector", None, None),
        P("term", "sector", None, None),
        P("term", "sector", None, None),
        P("term", "sector"),
        P("term", "sector"),
        P("sector", None),
        P(),
        P(),
    )
    out_specs = P("term", "sector", None, None)
    small = mesh.shape["sector"] == 4 and mesh.shape["term"] == 8

    def local(*args):
        return (direct if small else gathered)(*args)

    return jax.shard_map(local, mesh=mesh, in_specs=in_specs, out_specs=out_specs, check_vma=False)
```
